32 devices in a mesh: row: 8 (over y, x, core), col: 4 (over z).
Axes of the slice: x: 2, y: 2, z: 4, core: 2. Of those that a mesh axis runs over, the one named last changes fastest.
Arguments:
- coeffs: bfloat16 [6144, 4096], P('row', 'col'), may hold values from -0.00390625 to 0.00390625
- occupation: float32 [4096], P('col'), may hold values from 0.5 to 2
- basis_on_grid: bfloat16 [320, 512, 512], P('row'), may hold values from -6 to 6
- basis_map: int32 [320, 512], P('row'), may hold values from 0 to 6143, as said below
- basis_count: int32 [320], P('row'), may hold values from 256 to 512
- batch_atom: int32 [320], P('row'), may hold values from 0 to 63
- harmonics: float32 [320, 49, 512], P('row'), may hold values from -0.25 to 0.25
Outputs:
- density: float32 [320, 512], P('row', 'col')
- moments: float32 [64, 49], replicated
The draws below stay inside these ranges and needn't reach their ends.
Inputs may be any that keep to these rules, and one draw needn't show every extreme that they name: `basis_map`: the slots of one batch name distinct basis functions. With R = 768 and o = b // 40, batch b names only basis functions q * R + (o * 96 + w) mod R with 0 <= q < 8 and 0 <= w < 96.
All inputs are finite; a program needn't handle non-finite values.
Results may differ from the reference program's by a relative error of at most 0.0003.
Values may be sent and summed in bfloat16 or wider, within the bound.
A program may use at most 192 MiB of HBM per device.

```python
import jax
import jax.numpy as jnp
from jax import lax

NB = 6144
NOCC = 4096
SLOTS = 512
WIN = 96
POINTS = 512
LM = 49
NATOM = 64
BD = 40
BATCHES = 320


def draw_basis_map(key, part):
    owners = BATCHES // BD
    shard = NB // owners
    keys = jax.random.split(jax.random.fold_in(key, 7), BATCHES)
    chosen = jax.vmap(lambda one: jax.random.permutation(one, WIN * owners))(keys)[:, :SLOTS]
    chosen = chosen.astype(jnp.int32)
    source = chosen // WIN
    offset = chosen % WIN
    owner = jnp.arange(BATCHES, dtype=jnp.int32) // BD
    local = jnp.mod(owner[:, None] * WIN + offset, shard)
    return (source * shard + local).astype(jnp.int32)


def set_ends(values, own_key, low, high):
    longest = values.shape.index(max(values.shape))
    spots = []
    for shift in (0, 1):
        where = [jax.random.randint(jax.random.fold_in(own_key, axis), (), 0, length) for axis, length in enumerate(values.shape)]
        where[longest] = (where[longest] + shift) % values.shape[longest]
        spots.append(tuple(where))
    return values.at[spots[0]].set(low).at[spots[1]].set(high)


def block_scale(own_key, extent, cuts, smallest, largest):
    gain, own = 1.0, jax.random.fold_in(own_key, 6)
    for position, shards_of in cuts:
        heights = jnp.exp(jax.random.uniform(jax.random.fold_in(own, position), (shards_of,), jnp.float32, smallest / len(cuts), largest / len(cuts)))
        gain = gain * jnp.repeat(heights, extent[position] // shards_of).reshape([-1 if axis == position else 1 for axis in range(len(extent))])
    return gain


def centred(rng, extent, deviation, limit, pieces=(), held_as=jnp.bfloat16):
    factor_of = block_scale(rng, extent, pieces, -0.22, 0.18) if pieces else 1.0
    entries = jax.random.normal(rng, extent, jnp.float32) * deviation * factor_of
    return jnp.minimum(jnp.maximum(entries, -limit), limit).astype(held_as)


def setup_inputs(seed: int = 0) -> dict:
    seeds = jax.random.split(jax.random.key(seed), 8)
    return {
        "coeffs": centred(seeds[0], (NB, NOCC), (SLOTS * NOCC) ** -0.5, 0.00390625, ((0, 8), (1, 4))),
        "occupation": jnp.clip(0.5 + 1.5 * jax.random.uniform(seeds[1], (NOCC,), jnp.float32) ** block_scale(seeds[1], (NOCC,), ((0, 4),), -0.2, 0.2), 0.5, 2.0),
        "basis_on_grid": centred(seeds[2], (BATCHES, POINTS, SLOTS), 1.0, 6.0, ((0, 8),)),
        "basis_map": draw_basis_map(jax.random.fold_in(seeds[7], 71), 0),
        "basis_count": set_ends(jax.random.randint(seeds[4], (BATCHES,), SLOTS // 2, SLOTS + 1), jax.random.fold_in(seeds[4], 1), SLOTS // 2, SLOTS).astype(jnp.int32),
        "batch_atom": set_ends(jax.random.randint(seeds[5], (BATCHES,), 0, NATOM), jax.random.fold_in(seeds[5], 1), 0, NATOM - 1).astype(jnp.int32),
        "harmonics": centred(seeds[6], (BATCHES, LM, POINTS), POINTS ** -0.5, 0.25, ((0, 8),), jnp.float32),
    }


def reference(coeffs, occupation, basis_on_grid, basis_map, basis_count, batch_atom, harmonics):
    slot_ids = jnp.arange(SLOTS, dtype=jnp.int32)

    def one_batch(items):
        values, indices, count = items
        selected = jnp.take(coeffs, indices, axis=0)
        keep = slot_ids < count
        masked = jnp.where(keep[None, :], values, jnp.zeros_like(values))
        orbital = jnp.dot(masked, selected, preferred_element_type=jnp.float32)
        return jnp.sum(occupation[None, :] * orbital * orbital, axis=1)

    density = lax.map(one_batch, (basis_on_grid, basis_map, basis_count))
    local_moment = jnp.einsum("blp,bp->bl", harmonics, density, precision=lax.Precision.HIGHEST)
    member = (batch_atom[:, None] == jnp.arange(NATOM, dtype=jnp.int32)[None, :]).astype(jnp.float32)
    moments = jnp.dot(member.T, local_moment, precision=lax.Precision.HIGHEST)
    return density, moments
```

```python
import functools

import jax
import jax.numpy as jnp
from jax import lax
from jax.experimental import pallas as pl
from jax.experimental.pallas import tpu as pltpu
from jax.sharding import PartitionSpec as P

WIN = 96
NATOM = 64
VMEM_BYTES = 62 * 1024 * 1024
DEPTH = 3


def plain(coeffs, occupation, basis_on_grid, basis_map, basis_count, batch_atom, harmonics):
    batches, points, slots = basis_on_grid.shape
    owned = coeffs.shape[0]
    owners = lax.axis_size("row")
    target = lax.broadcasted_iota(jnp.int32, (owners, WIN), 0)
    offset = lax.broadcasted_iota(jnp.int32, (owners, WIN), 1)
    outgoing_ids = jnp.mod(target * WIN + offset, owned).reshape(-1)
    outgoing = jnp.take(coeffs, outgoing_ids, axis=0)
    window = lax.all_to_all(outgoing, "row", split_axis=0, concat_axis=0, tiled=True)
    start = jnp.mod(lax.axis_index("row") * WIN, owned)
    source = basis_map // owned
    within = jnp.mod(basis_map % owned - start, owned)
    local_ids = source * WIN + within
    selected = jnp.take(window, local_ids, axis=0)
    slot_ids = lax.broadcasted_iota(jnp.int32, (batches, slots), 1)
    keep = slot_ids < basis_count[:, None]
    masked = jnp.where(keep[:, None, :], basis_on_grid, jnp.zeros_like(basis_on_grid))
    orbital = jnp.einsum("bps,bsk->bpk", masked, selected, preferred_element_type=jnp.float32)
    partial_density = jnp.sum(orbital * orbital * occupation[None, None, :], axis=2)
    full_density = lax.psum(partial_density, "col")
    share = points // lax.axis_size("col")
    return lax.dynamic_slice_in_dim(full_density, lax.axis_index("col") * share, share, 1)


def kernel(rows, cols, owned, coeffs, occ, basis, index, count, out,
           held, window, across, weight, spread, dens, got,
           own_sem, in_sem, send_sem, recv_sem, dsend_sem, drecv_sem):
    batches, points, slots = basis.shape
    states = coeffs.shape[1]
    me, mine = lax.axis_index("row"), lax.axis_index("col")
    share = points // cols

    barrier = pltpu.get_barrier_semaphore()
    for k in range(1, rows):
        pl.semaphore_signal(barrier, inc=1, device_id={"row": lax.rem(me + k, rows)},
                            device_id_type=pl.DeviceIdType.MESH)
    for k in range(1, cols):
        pl.semaphore_signal(barrier, inc=1, device_id={"col": lax.rem(mine + k, cols)},
                            device_id_type=pl.DeviceIdType.MESH)

    def fetch(b, slot):
        return pltpu.make_async_copy(basis.at[b], held.at[slot], in_sem.at[slot])

    for b in range(DEPTH - 1):
        fetch(b, b).start()
    here = pl.ds(pl.multiple_of(me * WIN, 32), WIN)

    def rows_for(owner):
        return coeffs.at[pl.ds(pl.multiple_of(lax.rem(owner * WIN, owned), 32), WIN), :]

    own = pltpu.make_async_copy(rows_for(me), window.at[here, :], own_sem)
    own.start()
    pl.semaphore_wait(barrier, rows + cols - 2)
    sends = []
    for k in range(1, rows):
        peer = lax.rem(me + k, rows)
        copy = pltpu.make_async_remote_copy(
            src_ref=rows_for(peer), dst_ref=window.at[here, :],
            send_sem=send_sem.at[k - 1], recv_sem=recv_sem.at[k - 1],
            device_id={"row": peer}, device_id_type=pl.DeviceIdType.MESH)
        copy.start()
        sends.append(copy)

    for j in range(states // 128):
        line = jnp.broadcast_to(occ[j:j + 1, :], (128, 128))
        weight[j * 128:(j + 1) * 128, :] = line.T

    start = lax.rem(me * WIN, owned)
    row_of = lax.broadcasted_iota(jnp.int32, (WIN, 1), 0) + start
    name = jnp.concatenate([row_of + r * owned for r in range(rows)], axis=0)
    lane = lax.broadcasted_iota(jnp.int32, (1, slots), 1)

    def scatter(b, carry):
        slot = lax.rem(b, DEPTH)
        ahead = b + DEPTH - 1

        @pl.when(ahead < batches)
        def _():
            fetch(ahead, lax.rem(ahead, DEPTH)).start()

        fetch(b, slot).wait()
        ids = jnp.where(lane < count[b], index[pl.ds(b, 1), :], -1)
        hot = jnp.where(name == ids, 1.0, 0.0).astype(jnp.bfloat16)
        moved = lax.dot_general(hot, held[slot], (((1,), (1,)), ((), ())),
                                preferred_element_type=jnp.float32)
        spread[b] = moved.astype(jnp.bfloat16)
        return carry

    lax.fori_loop(0, batches, scatter, 0)

    own.wait()
    for copy in sends:
        copy.wait()
    for j in range(states // 128):
        across[j * 128:(j + 1) * 128, :] = window[:, j * 128:(j + 1) * 128].T

    def square(b, carry):
        values = spread[b]
        total = jnp.zeros((8, points), jnp.float32)
        step = 256
        for n in range(0, states, step):
            orbital = lax.dot_general(across[n:n + step, :], values, (((1,), (0,)), ((), ())),
                                      preferred_element_type=jnp.float32)
            scale = weight[n:n + step, :]
            scale = jnp.concatenate([scale] * (points // 128), axis=1)
            term = orbital * orbital * scale
            total = total + jnp.sum(term.reshape(step // 8, 8, points), axis=0)
        line = jnp.sum(total, axis=0, keepdims=True)
        for c in range(cols):
            dens[c, pl.ds(b, 1), :] = line[:, c * share:(c + 1) * share]
        return carry

    lax.fori_loop(0, batches, square, 0)

    copies = []
    for k in range(1, cols):
        peer = lax.rem(mine + k, cols)
        copy = pltpu.make_async_remote_copy(
            src_ref=dens.at[peer], dst_ref=got.at[k - 1],
            send_sem=dsend_sem.at[k - 1], recv_sem=drecv_sem.at[k - 1],
            device_id={"col": peer}, device_id_type=pl.DeviceIdType.MESH)
        copy.start()
        copies.append(copy)
    result = dens[mine]
    for k, copy in enumerate(copies):
        copy.wait()
        result = result + got[k]
    out[...] = result


def density_of(coeffs, occupation, basis_on_grid, basis_map, basis_count):
    batches, points, slots = basis_on_grid.shape
    owned, states = coeffs.shape
    rows, cols = lax.axis_size("row"), lax.axis_size("col")
    reach = rows * WIN
    vmem, dma = pltpu.VMEM, pltpu.SemaphoreType.DMA
    half, single = jnp.bfloat16, jnp.float32
    whole = pl.BlockSpec(memory_space=pltpu.VMEM)
    apart = pl.BlockSpec(memory_space=pl.ANY)
    return pl.pallas_call(
        functools.partial(kernel, rows, cols, owned),
        out_shape=jax.ShapeDtypeStruct((batches, points // cols), single),
        in_specs=[apart, whole, apart, whole, pl.BlockSpec(memory_space=pltpu.SMEM)],
        out_specs=whole,
        scratch_shapes=[
            vmem((DEPTH, points, slots), half),
            vmem((reach, states), half),
            vmem((states, reach), half),
            vmem((states, 128), single),
            vmem((batches, reach, points), half),
            vmem((cols, batches, points // cols), single),
            vmem((cols - 1, batches, points // cols), single),
            dma, dma((DEPTH,)), dma((rows - 1,)), dma((rows - 1,)),
            dma((cols - 1,)), dma((cols - 1,)),
        ],
        compiler_params=pltpu.CompilerParams(
            collective_id=0, has_side_effects=True, vmem_limit_bytes=VMEM_BYTES),
    )(coeffs, occupation.reshape(-1, 128), basis_on_grid, basis_map, basis_count)


def shards(coeffs, occupation, basis_on_grid, basis_map, basis_count, batch_atom, harmonics):
    batches, points, slots = basis_on_grid.shape
    owned, states = coeffs.shape
    cols, reach = lax.axis_size("col"), lax.axis_size("row") * WIN
    share = points // cols
    needed = batches * reach * points * 2 + 4 * reach * states
    if needed < VMEM_BYTES * 3 // 4 and share % 128 == 0 and owned % WIN == 0:
        density = density_of(coeffs, occupation, basis_on_grid, basis_map, basis_count)
    else:
        density = plain(coeffs, occupation, basis_on_grid, basis_map, basis_count,
                        batch_atom, harmonics)
    part = lax.dynamic_slice_in_dim(harmonics, lax.axis_index("col") * share, share, 2)
    local_moment = jnp.sum(part * density[:, None, :], axis=2)
    atom_ids = lax.broadcasted_iota(jnp.int32, (batches, NATOM), 1)
    member = (batch_atom[:, None] == atom_ids).astype(jnp.float32)
    atom_part = jnp.dot(member.T, local_moment, precision=lax.Precision.HIGHEST)
    moments = lax.psum(atom_part, ("row", "col"))
    return (density, moments)


def solution(mesh):
    placed = (
        P("row", "col"),
        P("col"),
        P("row", None, None),
        P("row", None),
        P("row"),
        P("row"),
        P("row", None, None),
    )
    return jax.shard_map(
        shards, mesh=mesh, in_specs=placed, out_specs=(P("row", "col"), P()), check_vma=False
    )
```

```python
import functools

import jax
import jax.numpy as jnp
from jax import lax
from jax.experimental import pallas as pl
from jax.experimental.pallas import tpu as pltpu
from jax.sharding import PartitionSpec as P

WIN = 96
NATOM = 64
VMEM_BYTES = 62 * 1024 * 1024
DEPTH = 3


def plain(coeffs, occupation, basis_on_grid, basis_map, basis_count):
    batches, points, slots = basis_on_grid.shape
    owned = coeffs.shape[0]
    owners = lax.axis_size("row")
    target = lax.broadcasted_iota(jnp.int32, (owners, WIN), 0)
    offset = lax.broadcasted_iota(jnp.int32, (owners, WIN), 1)
    outgoing_ids = jnp.mod(target * WIN + offset, owned).reshape(-1)
    outgoing = jnp.take(coeffs, outgoing_ids, axis=0)
    window = lax.all_to_all(outgoing, "row", split_axis=0, concat_axis=0, tiled=True)
    start = jnp.mod(lax.axis_index("row") * WIN, owned)
    source = basis_map // owned
    within = jnp.mod(basis_map % owned - start, owned)
    local_ids = source * WIN + within
    selected = jnp.take(window, local_ids, axis=0)
    slot_ids = lax.broadcasted_iota(jnp.int32, (batches, slots), 1)
    keep = slot_ids < basis_count[:, None]
    masked = jnp.where(keep[:, None, :], basis_on_grid, jnp.zeros_like(basis_on_grid))
    orbital = jnp.einsum("bps,bsk->bpk", masked, selected, preferred_element_type=jnp.float32)
    partial_density = jnp.sum(orbital * orbital * occupation[None, None, :], axis=2)
    full_density = lax.psum(partial_density, "col")
    share = points // lax.axis_size("col")
    return lax.dynamic_slice_in_dim(full_density, lax.axis_index("col") * share, share, 1)


def kernel(rows, cols, owned, coeffs, occ, basis, index, count, atom, harmonics, out, out_moments,
           held, window, across, weight, spread, angular, dens, got, near, far, moment,
           own_sem, in_sem, angular_sem, send_sem, recv_sem, dsend_sem, drecv_sem,
           nsend_sem, nrecv_sem, fsend_sem, frecv_sem):
    batches, points, slots = basis.shape
    states = coeffs.shape[1]
    me, mine = lax.axis_index("row"), lax.axis_index("col")
    share = points // cols

    barrier = pltpu.get_barrier_semaphore()
    for k in range(1, rows):
        pl.semaphore_signal(barrier, inc=1, device_id={"row": lax.rem(me + k, rows)},
                            device_id_type=pl.DeviceIdType.MESH)
    for k in range(1, cols):
        pl.semaphore_signal(barrier, inc=1, device_id={"col": lax.rem(mine + k, cols)},
                            device_id_type=pl.DeviceIdType.MESH)

    def fetch(b, slot):
        return pltpu.make_async_copy(basis.at[b], held.at[slot], in_sem.at[slot])

    for b in range(DEPTH - 1):
        fetch(b, b).start()
    here = pl.ds(pl.multiple_of(me * WIN, 32), WIN)

    def rows_for(owner):
        return coeffs.at[pl.ds(pl.multiple_of(lax.rem(owner * WIN, owned), 32), WIN), :]

    own = pltpu.make_async_copy(rows_for(me), window.at[here, :], own_sem)
    own.start()
    load = pltpu.make_async_copy(harmonics, angular, angular_sem)
    load.start()
    pl.semaphore_wait(barrier, rows + cols - 2)
    sends = []
    for k in range(1, rows):
        peer = lax.rem(me + k, rows)
        copy = pltpu.make_async_remote_copy(
            src_ref=rows_for(peer), dst_ref=window.at[here, :],
            send_sem=send_sem.at[k - 1], recv_sem=recv_sem.at[k - 1],
            device_id={"row": peer}, device_id_type=pl.DeviceIdType.MESH)
        copy.start()
        sends.append(copy)

    for j in range(states // 128):
        line = jnp.broadcast_to(occ[j:j + 1, :], (128, 128))
        weight[j * 128:(j + 1) * 128, :] = line.T

    start = lax.rem(me * WIN, owned)
    row_of = lax.broadcasted_iota(jnp.int32, (WIN, 1), 0) + start
    name = jnp.concatenate([row_of + r * owned for r in range(rows)], axis=0)
    lane = lax.broadcasted_iota(jnp.int32, (1, slots), 1)

    def scatter(b, carry):
        slot = lax.rem(b, DEPTH)
        ahead = b + DEPTH - 1

        @pl.when(ahead < batches)
        def _():
            fetch(ahead, lax.rem(ahead, DEPTH)).start()

        fetch(b, slot).wait()
        ids = jnp.where(lane < count[b], index[pl.ds(b, 1), :], -1)
        hot = jnp.where(name == ids, 1.0, 0.0).astype(jnp.bfloat16)
        moved = lax.dot_general(hot, held[slot], (((1,), (1,)), ((), ())),
                                preferred_element_type=jnp.float32)
        spread[b] = moved.astype(jnp.bfloat16)
        return carry

    lax.fori_loop(0, batches, scatter, 0)

    own.wait()
    for copy in sends:
        copy.wait()
    for j in range(states // 128):
        across[j * 128:(j + 1) * 128, :] = window[:, j * 128:(j + 1) * 128].T

    load.wait()
    moment[...] = jnp.zeros_like(moment)
    atoms = lax.broadcasted_iota(jnp.int32, (1, 128), 1)

    def square(b, carry):
        values = spread[b]
        total = jnp.zeros((8, points), jnp.float32)
        step = 256
        for n in range(0, states, step):
            orbital = lax.dot_general(across[n:n + step, :], values, (((1,), (0,)), ((), ())),
                                      preferred_element_type=jnp.float32)
            scale = weight[n:n + step, :]
            scale = jnp.concatenate([scale] * (points // 128), axis=1)
            term = orbital * orbital * scale
            total = total + jnp.sum(term.reshape(step // 8, 8, points), axis=0)
        line = jnp.sum(total, axis=0, keepdims=True)
        for c in range(cols):
            dens[c, pl.ds(b, 1), :] = line[:, c * share:(c + 1) * share]
        local = jnp.sum(angular[b] * line, axis=1, keepdims=True)
        moment[...] += local * jnp.where(atoms == atom[b], 1.0, 0.0)
        return carry

    lax.fori_loop(0, batches, square, 0)

    def exchange(axis, place, size, src_of, dst_of, sent, received):
        copies = []
        for k in range(1, size):
            peer = lax.rem(place + k, size)
            copy = pltpu.make_async_remote_copy(
                src_ref=src_of(peer), dst_ref=dst_of(k),
                send_sem=sent.at[k - 1], recv_sem=received.at[k - 1],
                device_id={axis: peer}, device_id_type=pl.DeviceIdType.MESH)
            copy.start()
            copies.append(copy)
        return copies

    moved = exchange("col", mine, cols, lambda peer: moment, lambda k: near.at[mine],
                     nsend_sem, nrecv_sem)
    copies = exchange("col", mine, cols, lambda peer: dens.at[peer], lambda k: got.at[k - 1],
                      dsend_sem, drecv_sem)
    near[mine] = moment[...]
    for copy in moved:
        copy.wait()
    total = near[0]
    for c in range(1, cols):
        total = total + near[c]
    moment[...] = total
    far[me] = total
    moved = exchange("row", me, rows, lambda peer: moment, lambda k: far.at[me],
                     fsend_sem, frecv_sem)
    result = dens[mine]
    for k, copy in enumerate(copies):
        copy.wait()
        result = result + got[k]
    out[...] = result
    for copy in moved:
        copy.wait()
    total = far[0]
    for r in range(1, rows):
        total = total + far[r]
    count_l = total.shape[0]
    total = jnp.concatenate([total, jnp.zeros((128 - count_l, 128), jnp.float32)], axis=0)
    out_moments[...] = total.T[:NATOM, :count_l]


def fused(coeffs, occupation, basis_on_grid, basis_map, basis_count, batch_atom, harmonics):
    batches, points, slots = basis_on_grid.shape
    owned, states = coeffs.shape
    rows, cols = lax.axis_size("row"), lax.axis_size("col")
    reach = rows * WIN
    vmem, dma = pltpu.VMEM, pltpu.SemaphoreType.DMA
    half, single = jnp.bfloat16, jnp.float32
    whole = pl.BlockSpec(memory_space=pltpu.VMEM)
    scalar = pl.BlockSpec(memory_space=pltpu.SMEM)
    lm = harmonics.shape[1]
    apart = pl.BlockSpec(memory_space=pl.ANY)
    return pl.pallas_call(
        functools.partial(kernel, rows, cols, owned),
        out_shape=(jax.ShapeDtypeStruct((batches, points // cols), single),
                   jax.ShapeDtypeStruct((NATOM, lm), single)),
        in_specs=[apart, whole, apart, whole, scalar, scalar, apart],
        out_specs=(whole, whole),
        scratch_shapes=[
            vmem((DEPTH, points, slots), half),
            vmem((reach, states), half),
            vmem((states, reach), half),
            vmem((states, 128), single),
            vmem((batches, reach, points), half),
            vmem((batches, lm, points), single),
            vmem((cols, batches, points // cols), single),
            vmem((cols - 1, batches, points // cols), single),
            vmem((cols, lm, 128), single),
            vmem((rows, lm, 128), single),
            vmem((lm, 128), single),
            dma, dma((DEPTH,)), dma, dma((rows - 1,)), dma((rows - 1,)),
            dma((cols - 1,)), dma((cols - 1,)), dma((cols - 1,)), dma((cols - 1,)),
            dma((rows - 1,)), dma((rows - 1,)),
        ],
        compiler_params=pltpu.CompilerParams(
            collective_id=0, has_side_effects=True, vmem_limit_bytes=VMEM_BYTES),
    )(coeffs, occupation.reshape(-1, 128), basis_on_grid, basis_map, basis_count,
      batch_atom, harmonics)


def shards(coeffs, occupation, basis_on_grid, basis_map, basis_count, batch_atom, harmonics):
    batches, points, slots = basis_on_grid.shape
    owned, states = coeffs.shape
    cols, reach = lax.axis_size("col"), lax.axis_size("row") * WIN
    share = points // cols
    needed = batches * reach * points * 2 + 4 * reach * states
    if needed < VMEM_BYTES * 3 // 4 and share % 128 == 0 and owned % WIN == 0:
        return fused(coeffs, occupation, basis_on_grid, basis_map, basis_count,
                     batch_atom, harmonics)
    density = plain(coeffs, occupation, basis_on_grid, basis_map, basis_count)
    part = lax.dynamic_slice_in_dim(harmonics, lax.axis_index("col") * share, share, 2)
    local_moment = jnp.sum(part * density[:, None, :], axis=2)
    atom_ids = lax.broadcasted_iota(jnp.int32, (batches, NATOM), 1)
    member = (batch_atom[:, None] == atom_ids).astype(jnp.float32)
    atom_part = jnp.dot(member.T, local_moment, precision=lax.Precision.HIGHEST)
    moments = lax.psum(atom_part, ("row", "col"))
    return (density, moments)


def solution(mesh):
    placed = (
        P("row", "col"),
        P("col"),
        P("row", None, None),
        P("row", None),
        P("row"),
        P("row"),
        P("row", None, None),
    )
    return jax.shard_map(
        shards, mesh=mesh, in_specs=placed, out_specs=(P("row", "col"), P()), check_vma=False
    )
```

```python
import functools

import jax
import jax.numpy as jnp
from jax import lax
from jax.experimental import pallas as pl
from jax.experimental.pallas import tpu as pltpu
from jax.sharding import PartitionSpec as P

WIN = 96
NATOM = 64
VMEM_BYTES = 62 * 1024 * 1024
HALVES = 2
DEPTH = 3


def plain(coeffs, occupation, basis_on_grid, basis_map, basis_count):
    batches, points, slots = basis_on_grid.shape
    owned = coeffs.shape[0]
    owners = lax.axis_size("row")
    target = lax.broadcasted_iota(jnp.int32, (owners, WIN), 0)
    offset = lax.broadcasted_iota(jnp.int32, (owners, WIN), 1)
    outgoing_ids = jnp.mod(target * WIN + offset, owned).reshape(-1)
    outgoing = jnp.take(coeffs, outgoing_ids, axis=0)
    window = lax.all_to_all(outgoing, "row", split_axis=0, concat_axis=0, tiled=True)
    start = jnp.mod(lax.axis_index("row") * WIN, owned)
    source = basis_map // owned
    within = jnp.mod(basis_map % owned - start, owned)
    local_ids = source * WIN + within
    selected = jnp.take(window, local_ids, axis=0)
    slot_ids = lax.broadcasted_iota(jnp.int32, (batches, slots), 1)
    keep = slot_ids < basis_count[:, None]
    masked = jnp.where(keep[:, None, :], basis_on_grid, jnp.zeros_like(basis_on_grid))
    orbital = jnp.einsum("bps,bsk->bpk", masked, selected, preferred_element_type=jnp.float32)
    partial_density = jnp.sum(orbital * orbital * occupation[None, None, :], axis=2)
    full_density = lax.psum(partial_density, "col")
    share = points // lax.axis_size("col")
    return lax.dynamic_slice_in_dim(full_density, lax.axis_index("col") * share, share, 1)


def kernel(rows, cols, owned, coeffs, occ, basis, index, count, atom, harmonics, out, out_moments,
           held, window, across, weight, spread, angular, dens, got, near, far, moment,
           own_sem, in_sem, angular_sem, send_sem, recv_sem, dsend_sem, drecv_sem,
           nsend_sem, nrecv_sem, fsend_sem, frecv_sem):
    batches, points, slots = basis.shape
    states = coeffs.shape[1]
    me, mine = lax.axis_index("row"), lax.axis_index("col")
    share = points // cols

    barrier = pltpu.get_barrier_semaphore()
    for k in range(1, rows):
        pl.semaphore_signal(barrier, inc=1, device_id={"row": lax.rem(me + k, rows)},
                            device_id_type=pl.DeviceIdType.MESH)
    for k in range(1, cols):
        pl.semaphore_signal(barrier, inc=1, device_id={"col": lax.rem(mine + k, cols)},
                            device_id_type=pl.DeviceIdType.MESH)

    def fetch(b, slot):
        return pltpu.make_async_copy(basis.at[b], held.at[slot], in_sem.at[slot])

    for b in range(DEPTH - 1):
        fetch(b, b).start()
    here = pl.ds(pl.multiple_of(me * WIN, 32), WIN)

    def rows_for(owner, columns=slice(None)):
        return coeffs.at[pl.ds(pl.multiple_of(lax.rem(owner * WIN, owned), 32), WIN), columns]

    own = pltpu.make_async_copy(rows_for(me), window.at[here, :], own_sem)
    own.start()
    load = pltpu.make_async_copy(harmonics, angular, angular_sem)
    load.start()
    pl.semaphore_wait(barrier, rows + cols - 2)
    width = states // HALVES
    sends = [[] for _ in range(HALVES)]
    for h in range(HALVES):
        columns = pl.ds(h * width, width)
        for k in range(1, rows):
            peer = lax.rem(me + k, rows)
            copy = pltpu.make_async_remote_copy(
                src_ref=rows_for(peer, columns), dst_ref=window.at[here, columns],
                send_sem=send_sem.at[h, k - 1], recv_sem=recv_sem.at[h, k - 1],
                device_id={"row": peer}, device_id_type=pl.DeviceIdType.MESH)
            copy.start()
            sends[h].append(copy)

    for j in range(states // 128):
        line = jnp.broadcast_to(occ[j:j + 1, :], (128, 128))
        weight[j * 128:(j + 1) * 128, :] = line.T

    start = lax.rem(me * WIN, owned)
    row_of = lax.broadcasted_iota(jnp.int32, (WIN, 1), 0) + start
    name = jnp.concatenate([row_of + r * owned for r in range(rows)], axis=0)
    lane = lax.broadcasted_iota(jnp.int32, (1, slots), 1)

    def scatter(b, carry):
        slot = lax.rem(b, DEPTH)
        ahead = b + DEPTH - 1

        @pl.when(ahead < batches)
        def _():
            fetch(ahead, lax.rem(ahead, DEPTH)).start()

        fetch(b, slot).wait()
        ids = jnp.where(lane < count[b], index[pl.ds(b, 1), :], -1)
        hot = jnp.where(name == ids, 1.0, 0.0).astype(jnp.bfloat16)
        moved = lax.dot_general(hot, held[slot], (((1,), (1,)), ((), ())),
                                preferred_element_type=jnp.float32)
        spread[b] = moved.astype(jnp.bfloat16)
        return carry

    lax.fori_loop(0, batches, scatter, 0)

    own.wait()
    load.wait()
    moment[...] = jnp.zeros_like(moment)
    atoms = lax.broadcasted_iota(jnp.int32, (1, 128), 1)

    def square(h, b, carry):
        values = spread[b]
        total = jnp.zeros((8, points), jnp.float32)
        step = 256
        for n in range(h * width, (h + 1) * width, step):
            orbital = lax.dot_general(across[n:n + step, :], values, (((1,), (0,)), ((), ())),
                                      preferred_element_type=jnp.float32)
            scale = weight[n:n + step, :]
            scale = jnp.concatenate([scale] * (points // 128), axis=1)
            term = orbital * orbital * scale
            total = total + jnp.sum(term.reshape(step // 8, 8, points), axis=0)
        line = jnp.sum(total, axis=0, keepdims=True)
        for c in range(cols):
            part = line[:, c * share:(c + 1) * share]
            dens[c, pl.ds(b, 1), :] = part if h == 0 else dens[c, pl.ds(b, 1), :] + part
        local = jnp.sum(angular[b] * line, axis=1, keepdims=True)
        moment[...] += local * jnp.where(atoms == atom[b], 1.0, 0.0)
        return carry

    for h in range(HALVES):
        for copy in sends[h]:
            copy.wait()
        for j in range(h * width // 128, (h + 1) * width // 128):
            across[j * 128:(j + 1) * 128, :] = window[:, j * 128:(j + 1) * 128].T
        lax.fori_loop(0, batches, functools.partial(square, h), 0)

    def exchange(axis, place, size, src_of, dst_of, sent, received):
        copies = []
        for k in range(1, size):
            peer = lax.rem(place + k, size)
            copy = pltpu.make_async_remote_copy(
                src_ref=src_of(peer), dst_ref=dst_of(k),
                send_sem=sent.at[k - 1], recv_sem=received.at[k - 1],
                device_id={axis: peer}, device_id_type=pl.DeviceIdType.MESH)
            copy.start()
            copies.append(copy)
        return copies

    moved = exchange("col", mine, cols, lambda peer: moment, lambda k: near.at[mine],
                     nsend_sem, nrecv_sem)
    copies = exchange("col", mine, cols, lambda peer: dens.at[peer], lambda k: got.at[k - 1],
                      dsend_sem, drecv_sem)
    near[mine] = moment[...]
    for copy in moved:
        copy.wait()
    total = near[0]
    for c in range(1, cols):
        total = total + near[c]
    moment[...] = total
    far[me] = total
    moved = exchange("row", me, rows, lambda peer: moment, lambda k: far.at[me],
                     fsend_sem, frecv_sem)
    result = dens[mine]
    for k, copy in enumerate(copies):
        copy.wait()
        result = result + got[k]
    out[...] = result
    for copy in moved:
        copy.wait()
    total = far[0]
    for r in range(1, rows):
        total = total + far[r]
    count_l = total.shape[0]
    total = jnp.concatenate([total, jnp.zeros((128 - count_l, 128), jnp.float32)], axis=0)
    out_moments[...] = total.T[:NATOM, :count_l]


def fused(coeffs, occupation, basis_on_grid, basis_map, basis_count, batch_atom, harmonics):
    batches, points, slots = basis_on_grid.shape
    owned, states = coeffs.shape
    rows, cols = lax.axis_size("row"), lax.axis_size("col")
    reach = rows * WIN
    vmem, dma = pltpu.VMEM, pltpu.SemaphoreType.DMA
    half, single = jnp.bfloat16, jnp.float32
    whole = pl.BlockSpec(memory_space=pltpu.VMEM)
    scalar = pl.BlockSpec(memory_space=pltpu.SMEM)
    lm = harmonics.shape[1]
    apart = pl.BlockSpec(memory_space=pl.ANY)
    return pl.pallas_call(
        functools.partial(kernel, rows, cols, owned),
        out_shape=(jax.ShapeDtypeStruct((batches, points // cols), single),
                   jax.ShapeDtypeStruct((NATOM, lm), single)),
        in_specs=[apart, whole, apart, whole, scalar, scalar, apart],
        out_specs=(whole, whole),
        scratch_shapes=[
            vmem((DEPTH, points, slots), half),
            vmem((reach, states), half),
            vmem((states, reach), half),
            vmem((states, 128), single),
            vmem((batches, reach, points), half),
            vmem((batches, lm, points), single),
            vmem((cols, batches, points // cols), single),
            vmem((cols - 1, batches, points // cols), single),
            vmem((cols, lm, 128), single),
            vmem((rows, lm, 128), single),
            vmem((lm, 128), single),
            dma, dma((DEPTH,)), dma, dma((HALVES, rows - 1)), dma((HALVES, rows - 1)),
            dma((cols - 1,)), dma((cols - 1,)), dma((cols - 1,)), dma((cols - 1,)),
            dma((rows - 1,)), dma((rows - 1,)),
        ],
        compiler_params=pltpu.CompilerParams(
            collective_id=0, has_side_effects=True, vmem_limit_bytes=VMEM_BYTES),
    )(coeffs, occupation.reshape(-1, 128), basis_on_grid, basis_map, basis_count,
      batch_atom, harmonics)


def shards(coeffs, occupation, basis_on_grid, basis_map, basis_count, batch_atom, harmonics):
    batches, points, slots = basis_on_grid.shape
    owned, states = coeffs.shape
    cols, reach = lax.axis_size("col"), lax.axis_size("row") * WIN
    share = points // cols
    needed = batches * reach * points * 2 + 4 * reach * states
    if needed < VMEM_BYTES * 3 // 4 and share % 128 == 0 and owned % WIN == 0:
        return fused(coeffs, occupation, basis_on_grid, basis_map, basis_count,
                     batch_atom, harmonics)
    density = plain(coeffs, occupation, basis_on_grid, basis_map, basis_count)
    part = lax.dynamic_slice_in_dim(harmonics, lax.axis_index("col") * share, share, 2)
    local_moment = jnp.sum(part * density[:, None, :], axis=2)
    atom_ids = lax.broadcasted_iota(jnp.int32, (batches, NATOM), 1)
    member = (batch_atom[:, None] == atom_ids).astype(jnp.float32)
    atom_part = jnp.dot(member.T, local_moment, precision=lax.Precision.HIGHEST)
    moments = lax.psum(atom_part, ("row", "col"))
    return (density, moments)


def solution(mesh):
    placed = (
        P("row", "col"),
        P("col"),
        P("row", None, None),
        P("row", None),
        P("row"),
        P("row"),
        P("row", None, None),
    )
    return jax.shard_map(
        shards, mesh=mesh, in_specs=placed, out_specs=(P("row", "col"), P()), check_vma=False
    )
```
